32 devices in a mesh: param: 16 (over z, x, core), qoi: 2 (over y).
Axes of the slice: x: 2, y: 2, z: 4, core: 2. Of those that a mesh axis runs over, the one named last changes fastest.
Arguments:
- samples: bfloat16 [16, 5120, 420], P('qoi', 'param'), may hold values from -6 to 6
- operator_rows: bfloat16 [8, 5120, 2, 512], P(None, 'param', None, 'qoi'), may hold values from -0.0625 to 0.0625
- block_start: int32 [1], replicated, may hold values from 0 to 203
- gauge_group: int32 [512], P('qoi'), may hold values from 0 to 15
Outputs:
- qoi_spectrum: float32 [16, 2, 8, 512], P('param', None, None, 'qoi')
- segment_response: float32 [16, 2, 8, 16], P('param')
The draws below stay inside these ranges and needn't reach their ends.
Inputs may be any that keep to these rules, and one draw needn't show every extreme that they name: `block_start`: the block's frequencies lie among the 211 frequencies of a real transform.
All inputs are finite; a program needn't handle non-finite values.
Results may differ from the reference program's by a relative error of at most 0.005.
Values may be sent and summed in bfloat16 or wider, within the bound.
A program may use at most 64 MiB of HBM per device.

```python
import math
import jax
import jax.numpy as jnp
from jax import lax

NF = 8
NT = 420
GROUPS = 16
SAMPLES = 16
NP = 5120
GAUGES = 512


def place_ends(result, rng, least, largest):
    longest = result.shape.index(max(result.shape))
    spots = []
    for shift in (0, 1):
        where = [jax.random.randint(jax.random.fold_in(rng, axis), (), 0, length) for axis, length in enumerate(result.shape)]
        where[longest] = (where[longest] + shift) % result.shape[longest]
        spots.append(tuple(where))
    return result.at[spots[0]].set(least).at[spots[1]].set(largest)


def raised(result, own_key, source, target, shards_of, factor):
    owner, partner = [(jnp.arange(result.shape[dim]) // (result.shape[dim] // shards_of)).reshape([-1 if axis == dim else 1 for axis in range(result.ndim)]) for dim in (source, target)]
    chosen = jax.random.permutation(own_key, shards_of)[partner]
    strong = (owner == chosen) | (owner == (partner + shards_of // 2) % shards_of)
    return jnp.where(strong, factor * result, result)


def block_scale(own_key, extent, split, least, largest):
    def one(dim, shards_of):
        steps = jax.random.uniform(jax.random.fold_in(jax.random.fold_in(own_key, 6), dim), (shards_of,), jnp.float32, least / len(split), largest / len(split))
        return jnp.repeat(jnp.exp(steps), extent[dim] // shards_of).reshape((-1,) + (1,) * (len(extent) - dim - 1))

    loudness = one(*split[0])
    for cut in split[1:]:
        loudness = loudness * one(*cut)
    return loudness


def noise(rng, shape, width, most, shards=(), held_as=jnp.bfloat16):
    loudness = block_scale(rng, shape, shards, -0.22, 0.18) if shards else 1.0
    drawn = jax.random.normal(rng, shape, jnp.float32) * width * loudness
    return jnp.minimum(jnp.maximum(drawn, -most), most).astype(held_as)


def gaussian_with(key, dims, scale, reach, split, heavy, kind=jnp.bfloat16):
    array = scale * jax.random.normal(key, dims, jnp.float32)
    if split:
        array = array * block_scale(key, dims, split, -0.22, 0.18)
    return jnp.clip(raised(array, jax.random.fold_in(key, 3), *heavy), -reach, reach).astype(kind)


def setup_inputs(seed: int = 0) -> dict:
    key_of = jax.random.split(jax.random.key(seed), 5)
    return {
        "samples": gaussian_with(key_of[0], (SAMPLES, NP, NT), 1.0, 6.0, ((0, 2), (1, 16)), (1, 0, 16, 2.0)),
        "operator_rows": noise(key_of[1], (NF, NP, 2, GAUGES), (2 * NP) ** -0.5, 0.0625, ((1, 16), (3, 2))),
        "block_start": jax.random.randint(key_of[2], (1,), 0, NT // 2 + 2 - NF).astype(jnp.int32),
        "gauge_group": place_ends(jax.random.randint(key_of[3], (GAUGES,), 0, GROUPS), jax.random.fold_in(key_of[3], 1), 0, GROUPS - 1).astype(jnp.int32),
    }


def sample_spectrum(series, first):
    spectrum_all = jnp.fft.rfft(series.astype(jnp.float32), axis=-1)
    window = lax.dynamic_slice_in_dim(spectrum_all, first, NF, 1)
    factor = 1.0 / math.sqrt(NT)
    real_part = (jnp.real(window) * factor).astype(jnp.bfloat16)
    imag_part = (jnp.imag(window) * factor).astype(jnp.bfloat16)
    return jnp.stack([real_part, imag_part], axis=0)

def frequency_response(paired):
    spectrum_f, weights_f = paired
    real_w = weights_f[:, 0, :]
    imag_w = weights_f[:, 1, :]
    real_real = jnp.dot(spectrum_f[0], real_w, preferred_element_type=jnp.float32)
    imag_imag = jnp.dot(spectrum_f[1], imag_w, preferred_element_type=jnp.float32)
    real_imag = jnp.dot(spectrum_f[0], imag_w, preferred_element_type=jnp.float32)
    imag_real = jnp.dot(spectrum_f[1], real_w, preferred_element_type=jnp.float32)
    return jnp.stack([real_real - imag_imag, real_imag + imag_real], axis=0)

def reference(samples, operator_rows, block_start, gauge_group):
    first = block_start[0].astype(jnp.int32)
    spectra = lax.map(lambda series: sample_spectrum(series, first), samples)
    spectra = jnp.transpose(spectra, (3, 1, 0, 2))
    responses = lax.map(frequency_response, (spectra, operator_rows))
    qoi_spectrum = jnp.transpose(responses, (2, 1, 0, 3))
    onehot = (gauge_group[:, None] == jnp.arange(GROUPS, dtype=jnp.int32)[None, :]).astype(jnp.float32)
    segment = jnp.dot(qoi_spectrum.reshape(-1, GAUGES), onehot, precision=lax.Precision.HIGHEST, preferred_element_type=jnp.float32)
    segment_response = segment.reshape(SAMPLES, 2, NF, GROUPS) * math.sqrt(GROUPS / GAUGES)
    return (qoi_spectrum, segment_response)
```

```python
import functools
import math

import jax
import jax.numpy as jnp
from jax import lax
from jax.experimental import pallas as pl
from jax.experimental.pallas import tpu as pltpu
from jax.sharding import PartitionSpec as P

GROUPS = 16
LANES = 128
CHUNKS = 2
PARTS = 2
MESH = pl.DeviceIdType.MESH
NT_DIMS = (((1,), (1,)), ((), ()))


def build_table(start, freq_count, steps_count, first, count, repeat):
    shape = (freq_count, count * repeat)
    steps = first + lax.broadcasted_iota(jnp.int32, shape, 1) // repeat
    freqs = lax.broadcasted_iota(jnp.int32, shape, 0) + start
    turns = (steps * freqs).astype(jnp.float32)
    whole = jnp.floor((turns + 0.5) * (1.0 / steps_count))
    phases = (turns - whole * steps_count) * (2.0 * math.pi / steps_count)
    table = jnp.concatenate([jnp.cos(phases), -jnp.sin(phases)], axis=0) * (
        1.0 / math.sqrt(steps_count)
    )
    high = table.astype(jnp.bfloat16).astype(jnp.float32)
    both = jnp.concatenate([high, table - high], axis=0)
    full = (4 * freq_count, repeat, count * repeat)
    keep = lax.broadcasted_iota(jnp.int32, full, 2) % repeat == lax.broadcasted_iota(
        jnp.int32, full, 1
    )
    wide = jnp.where(keep, both[:, None, :], 0.0)
    return wide.reshape(4 * freq_count * repeat, count * repeat).astype(jnp.bfloat16)


def spread(width):
    row = lax.broadcasted_iota(jnp.int32, (2 * width, 2 * width), 0)
    col = lax.broadcasted_iota(jnp.int32, (2 * width, 2 * width), 1)
    real = jnp.where(col == 2 * row, 1.0, 0.0)
    imag = jnp.where(col == 2 * (row - width) + 1, -1.0, 0.0)
    return jnp.where(row < width, real, imag).astype(jnp.bfloat16)


def swap():
    row = lax.broadcasted_iota(jnp.int32, (LANES, LANES), 0)
    col = lax.broadcasted_iota(jnp.int32, (LANES, LANES), 1)
    odd = col % 2
    value = jnp.where(odd == 1, 1.0, -1.0)
    return jnp.where(row == col + 1 - 2 * odd, value, 0.0).astype(jnp.bfloat16)


def kernel(
    param_count, qoi_count, start_hbm, group_ref, samples_hbm, rows_hbm,
    out_ref, seg_ref,
    start_ref, samples, weights, line, product, outgoing, incoming, total, segments,
    start_sem, samples_sem, weights_sem, line_send, line_recv, out_send, out_recv, seg_send, seg_recv,
):
    steps_count, sample_local, param_local = samples.shape
    freq_count, halves = weights.shape[0], weights.shape[1]
    gauge_local = halves * LANES
    sample_total = sample_local * qoi_count
    depth = 2 * param_local
    per_chunk = freq_count // CHUNKS
    me_p = lax.axis_index("param")
    me_q = lax.axis_index("qoi")

    barrier = pltpu.get_barrier_semaphore()
    for offset in range(1, qoi_count):
        pl.semaphore_signal(
            barrier, inc=1, device_id=(me_p, lax.rem(me_q + offset, qoi_count)), device_id_type=MESH
        )
    for offset in range(1, param_count):
        pl.semaphore_signal(
            barrier, inc=1, device_id=(lax.rem(me_p + offset, param_count), me_q), device_id_type=MESH
        )

    start_copy = pltpu.make_async_copy(start_hbm, start_ref, start_sem)
    start_copy.start()
    edges = [steps_count * part // PARTS // 32 * 32 for part in range(PARTS)] + [steps_count]
    sample_copies = []
    for part in range(PARTS):
        picked = pl.ds(edges[part], edges[part + 1] - edges[part])
        copy = pltpu.make_async_copy(
            samples_hbm.at[picked], samples.at[picked], samples_sem.at[part]
        )
        copy.start()
        sample_copies.append(copy)
    weight_copies = []
    for f in range(freq_count):
        for j in range(halves):
            copy = pltpu.make_async_copy(
                rows_hbm.at[f, :, :, pl.ds(j * LANES, LANES)],
                weights.at[f, j],
                weights_sem.at[f, j],
            )
            copy.start()
            weight_copies.append(copy)

    start_copy.wait()
    start = start_ref[0]
    swapper = swap()
    both = None
    for part in range(PARTS):
        first, count = edges[part], edges[part + 1] - edges[part]
        table = build_table(start, freq_count, steps_count, first, count, sample_local)
        sample_copies[part].wait()
        block = samples[pl.ds(first, count)].reshape(count * sample_local, param_local)
        term = jnp.dot(table, block, preferred_element_type=jnp.float32)
        both = term if both is None else both + term
    half = 2 * freq_count * sample_local
    spectrum = (both[:half] + both[half:]).astype(jnp.bfloat16)
    blocks = depth // LANES
    for base in range(0, param_local, LANES):
        width = min(LANES, param_local - base)
        pair = jnp.concatenate(
            [spectrum[: half // 2, base : base + width], spectrum[half // 2 :, base : base + width]],
            axis=1,
        )
        value = jnp.dot(pair, spread(width), preferred_element_type=jnp.float32)
        line[0, :, :, 2 * base : 2 * (base + width)] = (
            value.reshape(freq_count, sample_local, 2 * width).astype(jnp.bfloat16)
        )

    pl.semaphore_wait(barrier, qoi_count + param_count - 2)
    line_copies = []
    for chunk in range(CHUNKS):
        picked = pl.ds(chunk * per_chunk, per_chunk)
        for offset in range(1, qoi_count):
            copy = pltpu.make_async_remote_copy(
                src_ref=line.at[0, picked],
                dst_ref=line.at[offset, picked],
                send_sem=line_send.at[chunk, offset],
                recv_sem=line_recv.at[chunk, offset],
                device_id=(me_p, lax.rem(me_q + offset, qoi_count)),
                device_id_type=MESH,
            )
            copy.start()
            line_copies.append(copy)

    out_copies = []
    stripe = 2 * per_chunk
    for chunk in range(CHUNKS):
        for offset in range(1, qoi_count):
            line_copies[chunk * (qoi_count - 1) + offset - 1].wait_recv()
        for f in range(chunk * per_chunk, (chunk + 1) * per_chunk):
            real = jnp.concatenate([line[slot, f] for slot in range(qoi_count)], axis=0)
            stacked = jnp.concatenate(
                [real[:, b * LANES : (b + 1) * LANES] for b in range(blocks)], axis=0
            )
            turned = jnp.dot(stacked, swapper, preferred_element_type=jnp.float32).astype(
                jnp.bfloat16
            )
            imag = jnp.concatenate(
                [turned[b * sample_total : (b + 1) * sample_total] for b in range(blocks)], axis=1
            )
            left = jnp.concatenate([real, imag], axis=0)
            for j in range(halves):
                weight_copies[f * halves + j].wait()
            right = jnp.concatenate(
                [weights[f, j].reshape(depth, LANES) for j in range(halves)], axis=1
            )
            result = jnp.dot(left, right, preferred_element_type=jnp.float32)
            for j in range(halves):
                product[j, pl.ds(f * 2 * sample_total, 2 * sample_total), :] = result[
                    :, j * LANES : (j + 1) * LANES
                ]
        for r in range(sample_total):
            for j in range(halves):
                outgoing[r, chunk, :, j * LANES : (j + 1) * LANES] = product[
                    j,
                    pl.ds(chunk * per_chunk * 2 * sample_total + r, stripe, stride=sample_total),
                    :,
                ].astype(jnp.bfloat16)
        for offset in range(1, param_count):
            target = lax.rem(me_p + offset, param_count)
            slot = lax.rem(me_q + qoi_count - target // sample_local, qoi_count)
            place = slot * sample_local + lax.rem(target, sample_local)
            copy = pltpu.make_async_remote_copy(
                src_ref=outgoing.at[place, chunk],
                dst_ref=incoming.at[offset, chunk],
                send_sem=out_send.at[chunk, offset],
                recv_sem=out_recv.at[chunk, offset],
                device_id=(target, me_q),
                device_id_type=MESH,
            )
            copy.start()
            out_copies.append(copy)

    group_rows = lax.broadcasted_iota(jnp.int32, (LANES, gauge_local), 0)
    onehot = (group_rows == group_ref[...]).astype(jnp.float32)
    slot = lax.rem(me_q + qoi_count - me_p // sample_local, qoi_count)
    place = slot * sample_local + lax.rem(me_p, sample_local)
    for chunk in range(CHUNKS):
        partial = outgoing[place, chunk].astype(jnp.float32)
        for offset in range(1, param_count):
            out_copies[chunk * (param_count - 1) + offset - 1].wait_recv()
            partial = partial + incoming[offset, chunk].astype(jnp.float32)
        for j in range(halves):
            total[j, pl.ds(chunk * stripe, stripe), :] = partial[:, j * LANES : (j + 1) * LANES]
    ordered = jnp.concatenate(
        [
            jnp.concatenate(
                [total[j, pl.ds(part, freq_count, stride=2), :] for j in range(halves)], axis=1
            )
            for part in range(2)
        ],
        axis=0,
    )
    sums = lax.dot_general(
        ordered, onehot, NT_DIMS, precision=lax.Precision.HIGHEST,
        preferred_element_type=jnp.float32,
    )
    segments[me_q] = sums
    seg_copies = []
    for offset in range(1, qoi_count):
        copy = pltpu.make_async_remote_copy(
            src_ref=segments.at[me_q],
            dst_ref=segments.at[me_q],
            send_sem=seg_send.at[offset],
            recv_sem=seg_recv.at[offset],
            device_id=(me_p, lax.rem(me_q + offset, qoi_count)),
            device_id_type=MESH,
        )
        copy.start()
        seg_copies.append(copy)
    out_ref[...] = ordered.reshape(out_ref.shape)
    for copy in line_copies + out_copies:
        copy.wait_send()
    for copy in seg_copies:
        copy.wait()
    everything = segments[0]
    for q in range(1, qoi_count):
        everything = everything + segments[q]
    everything = everything * math.sqrt(GROUPS / (gauge_local * qoi_count))
    seg_ref[...] = everything[:, :GROUPS].reshape(seg_ref.shape)


def local(samples, operator_rows, block_start, gauge_group):
    sample_local, param_local, steps_count = samples.shape
    freq_count, _, _, gauge_local = operator_rows.shape
    param_count, qoi_count = lax.axis_size("param"), lax.axis_size("qoi")
    sample_total = sample_local * qoi_count
    halves = gauge_local // LANES
    depth = 2 * param_local
    stripe = 2 * freq_count // CHUNKS
    assert sample_total == param_count
    dma = pltpu.SemaphoreType.DMA
    vmem = pl.BlockSpec(memory_space=pltpu.VMEM)
    return pl.pallas_call(
        functools.partial(kernel, param_count, qoi_count),
        out_shape=(
            jax.ShapeDtypeStruct((1, 2, freq_count, gauge_local), jnp.float32),
            jax.ShapeDtypeStruct((1, 2, freq_count, GROUPS), jnp.float32),
        ),
        in_specs=[
            pl.BlockSpec(memory_space=pl.ANY),
            vmem,
            pl.BlockSpec(memory_space=pl.ANY),
            pl.BlockSpec(memory_space=pl.ANY),
        ],
        out_specs=(vmem, vmem),
        scratch_shapes=[
            pltpu.SMEM((1,), jnp.int32),
            pltpu.VMEM((steps_count, sample_local, param_local), jnp.bfloat16),
            pltpu.VMEM((freq_count, halves, param_local, 2, LANES), jnp.bfloat16),
            pltpu.VMEM((qoi_count, freq_count, sample_local, depth), jnp.bfloat16),
            pltpu.VMEM((halves, freq_count * 2 * sample_total, LANES), jnp.float32),
            pltpu.VMEM((sample_total, CHUNKS, stripe, gauge_local), jnp.bfloat16),
            pltpu.VMEM((param_count, CHUNKS, stripe, gauge_local), jnp.bfloat16),
            pltpu.VMEM((halves, 2 * freq_count, LANES), jnp.float32),
            pltpu.VMEM((qoi_count, 2 * freq_count, LANES), jnp.float32),
            dma(()),
            dma((PARTS,)),
            dma((freq_count, halves)),
            dma((CHUNKS, qoi_count)),
            dma((CHUNKS, qoi_count)),
            dma((CHUNKS, param_count)),
            dma((CHUNKS, param_count)),
            dma((qoi_count,)),
            dma((qoi_count,)),
        ],
        compiler_params=pltpu.CompilerParams(collective_id=0, has_side_effects=True),
    )(block_start, gauge_group.reshape(1, gauge_local), samples.transpose(2, 0, 1), operator_rows)


def solution(mesh):
    return jax.shard_map(
        local,
        mesh=mesh,
        in_specs=(P("qoi", "param", None), P(None, "param", None, "qoi"), P(), P("qoi")),
        out_specs=(P("param", None, None, "qoi"), P("param", None, None, None)),
        check_vma=False,
    )
```

```python
import functools
import math

import jax
import jax.numpy as jnp
from jax import lax
from jax.experimental import pallas as pl
from jax.experimental.pallas import tpu as pltpu
from jax.sharding import PartitionSpec as P

GROUPS = 16
LANES = 128
CHUNKS = 2
PARTS = 2
MESH = pl.DeviceIdType.MESH
NT_DIMS = (((1,), (1,)), ((), ()))


def build_table(start, freq_count, steps_count, first, count, repeat):
    shape = (freq_count, count * repeat)
    steps = first + lax.broadcasted_iota(jnp.int32, shape, 1) // repeat
    freqs = lax.broadcasted_iota(jnp.int32, shape, 0) + start
    turns = (steps * freqs).astype(jnp.float32)
    whole = jnp.floor((turns + 0.5) * (1.0 / steps_count))
    phases = (turns - whole * steps_count) * (2.0 * math.pi / steps_count)
    table = jnp.concatenate([jnp.cos(phases), -jnp.sin(phases)], axis=0) * (
        1.0 / math.sqrt(steps_count)
    )
    high = table.astype(jnp.bfloat16).astype(jnp.float32)
    both = jnp.concatenate([high, table - high], axis=0)
    full = (4 * freq_count, repeat, count * repeat)
    keep = lax.broadcasted_iota(jnp.int32, full, 2) % repeat == lax.broadcasted_iota(
        jnp.int32, full, 1
    )
    wide = jnp.where(keep, both[:, None, :], 0.0)
    return wide.reshape(4 * freq_count * repeat, count * repeat).astype(jnp.bfloat16)


def kernel(
    param_count, qoi_count, start_hbm, group_hbm, samples_hbm, rows_hbm,
    out_ref, seg_ref,
    start_ref, group_ref, samples, weights, loose, dense, line, product, outgoing, incoming, total, segments,
    start_sem, group_sem, samples_sem, weights_sem, line_send, line_recv, out_send, out_recv, seg_send, seg_recv,
):
    steps_count, sample_local, param_local = samples.shape
    freq_count = weights.shape[0]
    gauge_local = group_ref.shape[1]
    halves = gauge_local // LANES
    sample_total = sample_local * qoi_count
    depth = 2 * param_local
    per_chunk = freq_count // CHUNKS
    me_p = lax.axis_index("param")
    me_q = lax.axis_index("qoi")

    barrier = pltpu.get_barrier_semaphore()
    for offset in range(1, qoi_count):
        pl.semaphore_signal(
            barrier, inc=1, device_id=(me_p, lax.rem(me_q + offset, qoi_count)), device_id_type=MESH
        )
    for offset in range(1, param_count):
        pl.semaphore_signal(
            barrier, inc=1, device_id=(lax.rem(me_p + offset, param_count), me_q), device_id_type=MESH
        )

    start_copy = pltpu.make_async_copy(start_hbm, start_ref, start_sem)
    start_copy.start()
    group_copy = pltpu.make_async_copy(group_hbm, group_ref, group_sem)
    group_copy.start()
    edges = [steps_count * part // PARTS // 32 * 32 for part in range(PARTS)] + [steps_count]
    sample_copies = []
    for part in range(PARTS):
        picked = pl.ds(edges[part], edges[part + 1] - edges[part])
        copy = pltpu.make_async_copy(
            samples_hbm.at[picked], samples.at[picked], samples_sem.at[part]
        )
        copy.start()
        sample_copies.append(copy)
    start_copy.wait()
    start = start_ref[0]
    weight_copies = [
        pltpu.make_async_copy(rows_hbm.at[f], weights.at[f], weights_sem.at[f])
        for f in range(freq_count)
    ]
    both = None
    for part in range(PARTS):
        first, count = edges[part], edges[part + 1] - edges[part]
        table = build_table(start, freq_count, steps_count, first, count, sample_local)
        sample_copies[part].wait()
        if part == 0:
            for copy in weight_copies:
                copy.start()
        block = samples[pl.ds(first, count)].reshape(count * sample_local, param_local)
        term = jnp.dot(table, block, preferred_element_type=jnp.float32)
        both = term if both is None else both + term
    half = 2 * freq_count * sample_local
    spectrum = (both[:half] + both[half:]).astype(jnp.bfloat16)
    aligned = param_local // LANES * LANES
    parts = [spectrum[: half // 2], spectrum[half // 2 :]]
    pieces = [part[:, :aligned] for part in parts]
    if aligned < param_local:
        pieces.append(jnp.concatenate([part[:, aligned:] for part in parts], axis=1))
    line[0] = jnp.concatenate(pieces, axis=1).reshape(freq_count, sample_local, depth)

    pl.semaphore_wait(barrier, qoi_count + param_count - 2)
    line_copies = []
    for chunk in range(CHUNKS):
        picked = pl.ds(chunk * per_chunk, per_chunk)
        for offset in range(1, qoi_count):
            copy = pltpu.make_async_remote_copy(
                src_ref=line.at[0, picked],
                dst_ref=line.at[offset, picked],
                send_sem=line_send.at[chunk, offset],
                recv_sem=line_recv.at[chunk, offset],
                device_id=(me_p, lax.rem(me_q + offset, qoi_count)),
                device_id_type=MESH,
            )
            copy.start()
            line_copies.append(copy)

    for f in range(freq_count):
        weight_copies[f].wait()
        loose[...] = weights[f].astype(jnp.float32)
        for j in range(halves):
            parts = [
                loose[pl.ds(2 * j + part, param_local, stride=2 * halves), :].astype(jnp.bfloat16)
                for part in range(2)
            ]
            dense[f, :, j * LANES : (j + 1) * LANES] = jnp.concatenate(
                [part[:aligned] for part in parts] + [part[aligned:] for part in parts], axis=0
            )

    lane = lax.broadcasted_iota(jnp.int32, (1, depth), 1)
    tail = param_local - aligned
    second = ((lane >= aligned) & (lane < 2 * aligned)) | (lane >= 2 * aligned + tail)
    sign = jnp.where(second, -1.0, 1.0)
    out_copies = []
    stripe = 2 * per_chunk
    for chunk in range(CHUNKS):
        for offset in range(1, qoi_count):
            line_copies[chunk * (qoi_count - 1) + offset - 1].wait_recv()
        for f in range(chunk * per_chunk, (chunk + 1) * per_chunk):
            given = jnp.concatenate(
                [line[slot, f].astype(jnp.float32) for slot in range(qoi_count)], axis=0
            )
            real = given * sign
            swapped = [given[:, aligned : 2 * aligned], given[:, :aligned]]
            if tail:
                swapped.append(pltpu.roll(given[:, 2 * aligned :], tail, 1))
            left = jnp.concatenate([real, jnp.concatenate(swapped, axis=1)], axis=0)
            result = jnp.dot(
                left.astype(jnp.bfloat16), dense[f], preferred_element_type=jnp.float32
            )
            rows = 2 * sample_total
            for j in range(halves):
                product[j, pl.ds(f * rows, rows), :] = result[:, j * LANES : (j + 1) * LANES]
        for r in range(sample_total):
            for j in range(halves):
                outgoing[r, chunk, :, j * LANES : (j + 1) * LANES] = product[
                    j,
                    pl.ds(chunk * per_chunk * 2 * sample_total + r, stripe, stride=sample_total),
                    :,
                ].astype(jnp.bfloat16)
        for offset in range(1, param_count):
            target = lax.rem(me_p + offset, param_count)
            slot = lax.rem(me_q + qoi_count - target // sample_local, qoi_count)
            place = slot * sample_local + lax.rem(target, sample_local)
            copy = pltpu.make_async_remote_copy(
                src_ref=outgoing.at[place, chunk],
                dst_ref=incoming.at[offset, chunk],
                send_sem=out_send.at[chunk, offset],
                recv_sem=out_recv.at[chunk, offset],
                device_id=(target, me_q),
                device_id_type=MESH,
            )
            copy.start()
            out_copies.append(copy)

    group_copy.wait()
    group_rows = lax.broadcasted_iota(jnp.int32, (LANES, gauge_local), 0)
    onehot = (group_rows == group_ref[...]).astype(jnp.float32)
    slot = lax.rem(me_q + qoi_count - me_p // sample_local, qoi_count)
    place = slot * sample_local + lax.rem(me_p, sample_local)
    for chunk in range(CHUNKS):
        partial = outgoing[place, chunk].astype(jnp.float32)
        for offset in range(1, param_count):
            out_copies[chunk * (param_count - 1) + offset - 1].wait_recv()
            partial = partial + incoming[offset, chunk].astype(jnp.float32)
        for j in range(halves):
            total[j, pl.ds(chunk * stripe, stripe), :] = partial[:, j * LANES : (j + 1) * LANES]
    ordered = jnp.concatenate(
        [
            jnp.concatenate(
                [total[j, pl.ds(part, freq_count, stride=2), :] for j in range(halves)], axis=1
            )
            for part in range(2)
        ],
        axis=0,
    )
    sums = lax.dot_general(
        ordered, onehot, NT_DIMS, precision=lax.Precision.HIGHEST,
        preferred_element_type=jnp.float32,
    )
    segments[me_q] = sums
    seg_copies = []
    for offset in range(1, qoi_count):
        copy = pltpu.make_async_remote_copy(
            src_ref=segments.at[me_q],
            dst_ref=segments.at[me_q],
            send_sem=seg_send.at[offset],
            recv_sem=seg_recv.at[offset],
            device_id=(me_p, lax.rem(me_q + offset, qoi_count)),
            device_id_type=MESH,
        )
        copy.start()
        seg_copies.append(copy)
    out_ref[...] = ordered.reshape(out_ref.shape)
    for copy in line_copies + out_copies:
        copy.wait_send()
    for copy in seg_copies:
        copy.wait()
    everything = segments[0]
    for q in range(1, qoi_count):
        everything = everything + segments[q]
    everything = everything * math.sqrt(GROUPS / (gauge_local * qoi_count))
    seg_ref[...] = everything[:, :GROUPS].reshape(seg_ref.shape)


def local(samples, operator_rows, block_start, gauge_group):
    sample_local, param_local, steps_count = samples.shape
    freq_count, _, _, gauge_local = operator_rows.shape
    param_count, qoi_count = lax.axis_size("param"), lax.axis_size("qoi")
    sample_total = sample_local * qoi_count
    halves = gauge_local // LANES
    depth = 2 * param_local
    stripe = 2 * freq_count // CHUNKS
    assert sample_total == param_count
    rows = operator_rows.reshape(freq_count, param_local, 2, halves, LANES)
    rows = rows.transpose(0, 1, 3, 2, 4).reshape(freq_count, depth * halves, LANES)
    dma = pltpu.SemaphoreType.DMA
    vmem = pl.BlockSpec(memory_space=pltpu.VMEM)
    hbm = pl.BlockSpec(memory_space=pltpu.HBM)
    return pl.pallas_call(
        functools.partial(kernel, param_count, qoi_count),
        out_shape=(
            jax.ShapeDtypeStruct((1, 2, freq_count, gauge_local), jnp.float32),
            jax.ShapeDtypeStruct((1, 2, freq_count, GROUPS), jnp.float32),
        ),
        in_specs=[
            pl.BlockSpec(memory_space=pl.ANY),
            hbm,
            hbm,
            hbm,
        ],
        out_specs=(vmem, vmem),
        scratch_shapes=[
            pltpu.SMEM((1,), jnp.int32),
            pltpu.VMEM((1, gauge_local), jnp.int32),
            pltpu.VMEM((steps_count, sample_local, param_local), jnp.bfloat16),
            pltpu.VMEM((freq_count, depth * halves, LANES), jnp.bfloat16),
            pltpu.VMEM((depth * halves, LANES), jnp.float32),
            pltpu.VMEM((freq_count, depth, gauge_local), jnp.bfloat16),
            pltpu.VMEM((qoi_count, freq_count, sample_local, depth), jnp.bfloat16),
            pltpu.VMEM((halves, freq_count * 2 * sample_total, LANES), jnp.float32),
            pltpu.VMEM((sample_total, CHUNKS, stripe, gauge_local), jnp.bfloat16),
            pltpu.VMEM((param_count, CHUNKS, stripe, gauge_local), jnp.bfloat16),
            pltpu.VMEM((halves, 2 * freq_count, LANES), jnp.float32),
            pltpu.VMEM((qoi_count, 2 * freq_count, LANES), jnp.float32),
            dma(()),
            dma(()),
            dma((PARTS,)),
            dma((freq_count,)),
            dma((CHUNKS, qoi_count)),
            dma((CHUNKS, qoi_count)),
            dma((CHUNKS, param_count)),
            dma((CHUNKS, param_count)),
            dma((qoi_count,)),
            dma((qoi_count,)),
        ],
        compiler_params=pltpu.CompilerParams(collective_id=0, has_side_effects=True, vmem_limit_bytes=53 * 2**20),
    )(block_start, gauge_group.reshape(1, gauge_local), samples.transpose(2, 0, 1), rows)


def solution(mesh):
    return jax.shard_map(
        local,
        mesh=mesh,
        in_specs=(P("qoi", "param", None), P(None, "param", None, "qoi"), P(), P("qoi")),
        out_specs=(P("param", None, None, "qoi"), P("param", None, None, None)),
        check_vma=False,
    )
```

```python
import functools
import math

import jax
import jax.numpy as jnp
from jax import lax
from jax.experimental import pallas as pl
from jax.experimental.pallas import tpu as pltpu
from jax.sharding import PartitionSpec as P

GROUPS = 16
LANES = 128
CHUNKS = 1
PARTS = 2
MESH = pl.DeviceIdType.MESH
NT_DIMS = (((1,), (1,)), ((), ()))


def build_table(start, freq_count, steps_count, first, count, repeat):
    shape = (freq_count, count * repeat)
    steps = first + lax.broadcasted_iota(jnp.int32, shape, 1) // repeat
    freqs = lax.broadcasted_iota(jnp.int32, shape, 0) + start
    turns = (steps * freqs).astype(jnp.float32)
    whole = jnp.floor((turns + 0.5) * (1.0 / steps_count))
    phases = (turns - whole * steps_count) * (2.0 * math.pi / steps_count)
    table = jnp.concatenate([jnp.cos(phases), -jnp.sin(phases)], axis=0) * (
        1.0 / math.sqrt(steps_count)
    )
    high = table.astype(jnp.bfloat16).astype(jnp.float32)
    both = jnp.concatenate([high, table - high], axis=0)
    full = (4 * freq_count, repeat, count * repeat)
    keep = lax.broadcasted_iota(jnp.int32, full, 2) % repeat == lax.broadcasted_iota(
        jnp.int32, full, 1
    )
    wide = jnp.where(keep, both[:, None, :], 0.0)
    return wide.reshape(4 * freq_count * repeat, count * repeat).astype(jnp.bfloat16)


def kernel(
    param_count, qoi_count, start_hbm, group_hbm, samples_hbm, rows_hbm,
    out_ref, seg_ref,
    start_ref, group_ref, samples, weights, loose, dense, hot, line, product, outgoing, incoming, total, joined, shares, gathered,
    start_sem, group_sem, samples_sem, weights_sem, line_send, line_recv, out_send, out_recv, share_send, share_recv,
):
    steps_count, sample_local, param_local = samples.shape
    freq_count = weights.shape[0]
    gauge_local = group_ref.shape[1]
    halves = gauge_local // LANES
    sample_total = sample_local * qoi_count
    depth = 2 * param_local
    per_chunk = freq_count // CHUNKS
    me_p = lax.axis_index("param")
    me_q = lax.axis_index("qoi")

    barrier = pltpu.get_barrier_semaphore()
    for far in range(qoi_count):
        for offset in range(param_count):
            if far or offset:
                pl.semaphore_signal(
                    barrier,
                    inc=1,
                    device_id=(
                        lax.rem(me_p + offset, param_count), lax.rem(me_q + far, qoi_count)
                    ),
                    device_id_type=MESH,
                )

    start_copy = pltpu.make_async_copy(start_hbm, start_ref, start_sem)
    start_copy.start()
    group_copy = pltpu.make_async_copy(group_hbm, group_ref, group_sem)
    group_copy.start()
    edges = [steps_count * part // PARTS // 32 * 32 for part in range(PARTS)] + [steps_count]
    sample_copies = []
    for part in range(PARTS):
        picked = pl.ds(edges[part], edges[part + 1] - edges[part])
        copy = pltpu.make_async_copy(
            samples_hbm.at[picked], samples.at[picked], samples_sem.at[part]
        )
        copy.start()
        sample_copies.append(copy)
    start_copy.wait()
    start = start_ref[0]
    weight_copies = [
        pltpu.make_async_copy(rows_hbm.at[f], weights.at[f], weights_sem.at[f])
        for f in range(freq_count)
    ]
    both = None
    for part in range(PARTS):
        first, count = edges[part], edges[part + 1] - edges[part]
        table = build_table(start, freq_count, steps_count, first, count, sample_local)
        sample_copies[part].wait()
        if part == 0:
            for copy in weight_copies:
                copy.start()
        block = samples[pl.ds(first, count)].reshape(count * sample_local, param_local)
        term = jnp.dot(table, block, preferred_element_type=jnp.float32)
        both = term if both is None else both + term
    half = 2 * freq_count * sample_local
    spectrum = (both[:half] + both[half:]).astype(jnp.bfloat16)
    aligned = param_local // LANES * LANES
    parts = [spectrum[: half // 2], spectrum[half // 2 :]]
    pieces = [part[:, :aligned] for part in parts]
    if aligned < param_local:
        pieces.append(jnp.concatenate([part[:, aligned:] for part in parts], axis=1))
    line[me_q] = jnp.concatenate(pieces, axis=1).reshape(freq_count, sample_local, depth)

    pl.semaphore_wait(barrier, qoi_count * param_count - 1)
    line_copies = []
    for chunk in range(CHUNKS):
        picked = pl.ds(chunk * per_chunk, per_chunk)
        for offset in range(1, qoi_count):
            copy = pltpu.make_async_remote_copy(
                src_ref=line.at[me_q, picked],
                dst_ref=line.at[me_q, picked],
                send_sem=line_send.at[chunk, offset],
                recv_sem=line_recv.at[chunk, offset],
                device_id=(me_p, lax.rem(me_q + offset, qoi_count)),
                device_id_type=MESH,
            )
            copy.start()
            line_copies.append(copy)

    for f in range(freq_count):
        weight_copies[f].wait()
        loose[...] = weights[f].astype(jnp.float32)
        for j in range(halves):
            parts = [
                loose[pl.ds(2 * j + part, param_local, stride=2 * halves), :].astype(jnp.bfloat16)
                for part in range(2)
            ]
            dense[f, :, j * LANES : (j + 1) * LANES] = jnp.concatenate(
                [part[:aligned] for part in parts] + [part[aligned:] for part in parts], axis=0
            )

    group_copy.wait()
    columns = lax.broadcasted_iota(jnp.int32, (LANES, gauge_local), 0)
    for f in range(freq_count):
        hot[f] = (columns == group_ref[...] + f * GROUPS).astype(jnp.float32).astype(jnp.bfloat16)

    lane = lax.broadcasted_iota(jnp.int32, (1, depth), 1)
    tail = param_local - aligned
    second = ((lane >= aligned) & (lane < 2 * aligned)) | (lane >= 2 * aligned + tail)
    sign = jnp.where(second, -1.0, 1.0)
    out_copies = []
    order = list(range(1, param_count))
    stripe = 2 * per_chunk
    for chunk in range(CHUNKS):
        for offset in range(1, qoi_count):
            line_copies[chunk * (qoi_count - 1) + offset - 1].wait_recv()
        for f in range(chunk * per_chunk, (chunk + 1) * per_chunk):
            given = jnp.concatenate(
                [line[slot, f].astype(jnp.float32) for slot in range(qoi_count)], axis=0
            )
            real = given * sign
            swapped = [given[:, aligned : 2 * aligned], given[:, :aligned]]
            if tail:
                swapped.append(pltpu.roll(given[:, 2 * aligned :], tail, 1))
            left = jnp.concatenate([real, jnp.concatenate(swapped, axis=1)], axis=0)
            result = jnp.dot(
                left.astype(jnp.bfloat16), dense[f], preferred_element_type=jnp.float32
            )
            rows = 2 * sample_total
            sums = lax.dot_general(
                result.astype(jnp.bfloat16), hot[f], NT_DIMS, preferred_element_type=jnp.float32
            )
            segment = sums if f == 0 else segment + sums
            for j in range(halves):
                product[j, pl.ds(f * rows, rows), :] = result[:, j * LANES : (j + 1) * LANES]
        for r in range(sample_total):
            for j in range(halves):
                outgoing[r, chunk, :, j * LANES : (j + 1) * LANES] = product[
                    j,
                    pl.ds(chunk * per_chunk * 2 * sample_total + r, stripe, stride=sample_total),
                    :,
                ].astype(jnp.bfloat16)
        if chunk == CHUNKS - 1:
            joined[...] = segment * math.sqrt(GROUPS / (gauge_local * qoi_count))
            for k in range(sample_total):
                shares[k] = joined[pl.ds(k, 2, stride=sample_total), :]
            mine = me_q * param_count + me_p
            gathered[mine] = shares[me_p]
            seg_copies = []
            for far in reversed(range(qoi_count)):
                for offset in order + [0]:
                    if far == 0 and offset == 0:
                        continue
                    target = lax.rem(me_p + offset, param_count)
                    copy = pltpu.make_async_remote_copy(
                        src_ref=shares.at[target],
                        dst_ref=gathered.at[mine],
                        send_sem=share_send.at[far * param_count + offset],
                        recv_sem=share_recv.at[far * param_count + offset],
                        device_id=(target, lax.rem(me_q + far, qoi_count)),
                        device_id_type=MESH,
                    )
                    copy.start()
                    seg_copies.append(copy)
        for offset in order:
            target = lax.rem(me_p + offset, param_count)
            copy = pltpu.make_async_remote_copy(
                src_ref=outgoing.at[target, chunk],
                dst_ref=incoming.at[offset, chunk],
                send_sem=out_send.at[chunk, offset],
                recv_sem=out_recv.at[chunk, offset],
                device_id=(target, me_q),
                device_id_type=MESH,
            )
            copy.start()
            out_copies.append(copy)

    for chunk in range(CHUNKS):
        partial = outgoing[me_p, chunk].astype(jnp.float32)
        for index, offset in reversed(list(enumerate(order))):
            out_copies[chunk * (param_count - 1) + index].wait_recv()
            partial = partial + incoming[offset, chunk].astype(jnp.float32)
        for j in range(halves):
            total[j, pl.ds(chunk * stripe, stripe), :] = partial[:, j * LANES : (j + 1) * LANES]
    ordered = jnp.concatenate(
        [
            jnp.concatenate(
                [total[j, pl.ds(part, freq_count, stride=2), :] for j in range(halves)], axis=1
            )
            for part in range(2)
        ],
        axis=0,
    )
    out_ref[...] = ordered.reshape(out_ref.shape)
    for copy in line_copies + out_copies:
        copy.wait_send()
    for copy in seg_copies:
        copy.wait()
    final = gathered[0]
    for p in range(1, param_count * qoi_count):
        final = final + gathered[p]
    seg_ref[...] = final.reshape(seg_ref.shape)


def local(samples, operator_rows, block_start, gauge_group):
    sample_local, param_local, steps_count = samples.shape
    freq_count, _, _, gauge_local = operator_rows.shape
    param_count, qoi_count = lax.axis_size("param"), lax.axis_size("qoi")
    sample_total = sample_local * qoi_count
    halves = gauge_local // LANES
    depth = 2 * param_local
    stripe = 2 * freq_count // CHUNKS
    assert sample_total == param_count and freq_count * GROUPS == LANES
    rows = operator_rows.reshape(freq_count, param_local, 2, halves, LANES)
    rows = rows.transpose(0, 1, 3, 2, 4).reshape(freq_count, depth * halves, LANES)
    dma = pltpu.SemaphoreType.DMA
    vmem = pl.BlockSpec(memory_space=pltpu.VMEM)
    hbm = pl.BlockSpec(memory_space=pltpu.HBM)
    qoi_spectrum, response = pl.pallas_call(
        functools.partial(kernel, param_count, qoi_count),
        out_shape=(
            jax.ShapeDtypeStruct((1, 2, freq_count, gauge_local), jnp.float32),
            jax.ShapeDtypeStruct((1, 2, freq_count * GROUPS), jnp.float32),
        ),
        in_specs=[
            pl.BlockSpec(memory_space=pl.ANY),
            hbm,
            hbm,
            hbm,
        ],
        out_specs=(vmem, vmem),
        scratch_shapes=[
            pltpu.SMEM((1,), jnp.int32),
            pltpu.VMEM((1, gauge_local), jnp.int32),
            pltpu.VMEM((steps_count, sample_local, param_local), jnp.bfloat16),
            pltpu.VMEM((freq_count, depth * halves, LANES), jnp.bfloat16),
            pltpu.VMEM((depth * halves, LANES), jnp.float32),
            pltpu.VMEM((freq_count, depth, gauge_local), jnp.bfloat16),
            pltpu.VMEM((freq_count, LANES, gauge_local), jnp.bfloat16),
            pltpu.VMEM((qoi_count, freq_count, sample_local, depth), jnp.bfloat16),
            pltpu.VMEM((halves, freq_count * 2 * sample_total, LANES), jnp.float32),
            pltpu.VMEM((sample_total, CHUNKS, stripe, gauge_local), jnp.bfloat16),
            pltpu.VMEM((param_count, CHUNKS, stripe, gauge_local), jnp.bfloat16),
            pltpu.VMEM((halves, 2 * freq_count, LANES), jnp.float32),
            pltpu.VMEM((2 * sample_total, LANES), jnp.float32),
            pltpu.VMEM((sample_total, 2, LANES), jnp.float32),
            pltpu.VMEM((qoi_count * param_count, 2, LANES), jnp.float32),
            dma(()),
            dma(()),
            dma((PARTS,)),
            dma((freq_count,)),
            dma((CHUNKS, qoi_count)),
            dma((CHUNKS, qoi_count)),
            dma((CHUNKS, param_count)),
            dma((CHUNKS, param_count)),
            dma((qoi_count * param_count,)),
            dma((qoi_count * param_count,)),
        ],
        compiler_params=pltpu.CompilerParams(collective_id=0, has_side_effects=True, vmem_limit_bytes=53 * 2**20),
    )(block_start, gauge_group.reshape(1, gauge_local), samples.transpose(2, 0, 1), rows)
    return qoi_spectrum, response.reshape(1, 2, freq_count, GROUPS)


def solution(mesh):
    return jax.shard_map(
        local,
        mesh=mesh,
        in_specs=(P("qoi", "param", None), P(None, "param", None, "qoi"), P(), P("qoi")),
        out_specs=(P("param", None, None, "qoi"), P("param", None, None, None)),
        check_vma=False,
    )
```
